8 devices in a mesh: batch: 2 (over z, y), t: 4 (over x, core).
Axes of the slice: x: 2, y: 2, z: 1, core: 2. Of those that a mesh axis runs over, the one named last changes fastest.
Arguments:
- z: bfloat16 [16, 32, 64, 256], P(('batch', 't')), parts along dimension 0
- w: bfloat16 [5, 3, 3, 3, 256, 256], replicated
- b: float32 [5, 256], replicated
- gamma: float32 [4, 256], replicated
- beta: float32 [4, 256], replicated
Outputs:
- output: bfloat16 [32, 64, 128, 256], P(('batch', 't')), parts along dimension 0
There are 2 independent parts. The reference program is written for one: setup_inputs(seed, part) draws one part's arguments, and reference() takes and returns one part's arrays. A program takes and returns all parts, laid end to end along the dimension named above; an argument that names none is the same for every part.
All inputs are finite; a program needn't handle non-finite values.
Results may differ from the reference program's by a relative error of at most 0.0150017.
Values are sent between devices in bfloat16 or wider.
A program may use at most 1 GiB of HBM per device.

```python
import jax
import jax.numpy as jnp
from jax import lax

T = 8
H = 32
W = 64
C = 256
GROUPS = 32
EPS = 1e-6
DN = ('NDHWC', 'DHWIO', 'NDHWC')


def setup_inputs(seed: int = 0, part: int = 0) -> dict:
    key = jax.random.key(seed)
    kz, ka, km = jax.random.split(jax.random.fold_in(key, part), 3)
    kw, kb, kg, kbe = jax.random.split(key, 4)
    amp = jnp.exp(0.5 * jax.random.normal(ka, (T, 1, 1, 1), jnp.float32))
    ramp = jnp.linspace(-1.0, 1.0, T)[:, None, None, None]
    mean = ramp * jax.random.normal(km, (1, 1, 1, C), jnp.float32)
    z = amp * jax.random.normal(kz, (T, H, W, C), jnp.float32) + mean
    w = jax.random.normal(kw, (5, 3, 3, 3, C, C), jnp.float32) * (27 * C) ** -0.5
    b = 0.1 * jax.random.normal(kb, (5, C), jnp.float32)
    gamma = 1.0 + 0.2 * jax.random.normal(kg, (4, C), jnp.float32)
    beta = 0.2 * jax.random.normal(kbe, (4, C), jnp.float32)
    return {'z': z.astype(jnp.bfloat16), 'w': w.astype(jnp.bfloat16), 'b': b, 'gamma': gamma, 'beta': beta}


def _conv(x, wk, bk):
    xp = jnp.concatenate([x[:1], x[:1], x], axis=0).astype(jnp.float32)
    y = lax.conv_general_dilated(xp[None], wk.astype(jnp.float32), (1, 1, 1), ((0, 0), (1, 1), (1, 1)), dimension_numbers=DN)[0]
    return (y + bk).astype(jnp.bfloat16)


def _norm_act(x, g, be):
    xf = x.astype(jnp.float32).reshape(x.shape[:-1] + (GROUPS, x.shape[-1] // GROUPS))
    cnt = xf.size // GROUPS
    mean = jnp.sum(xf, axis=(0, 1, 2, 4)) / cnt
    var = jnp.sum(xf * xf, axis=(0, 1, 2, 4)) / cnt - mean * mean
    xn = ((xf - mean[:, None]) * lax.rsqrt(var + EPS)[:, None]).reshape(x.shape) * g + be
    xn = xn.astype(jnp.bfloat16).astype(jnp.float32)
    return jax.nn.silu(xn).astype(jnp.bfloat16)


def _resblock(x, w, b, gamma, beta, i, j):
    h = _conv(_norm_act(x, gamma[i], beta[i]), w[j], b[j])
    h = _conv(_norm_act(h, gamma[i + 1], beta[i + 1]), w[j + 1], b[j + 1])
    return (x.astype(jnp.float32) + h.astype(jnp.float32)).astype(jnp.bfloat16)


def _upsample(x):
    x = jnp.repeat(jnp.repeat(x, 2, axis=1), 2, axis=2)
    return jnp.concatenate([x[:1], jnp.repeat(x[1:], 2, axis=0)], axis=0)


def reference(z, w, b, gamma, beta):
    x = _resblock(z, w, b, gamma, beta, 0, 0)
    u = _conv(_upsample(x), w[2], b[2])
    y = _resblock(u, w, b, gamma, beta, 2, 3)
    return jnp.concatenate([y[:1], y], axis=0)
```

```python
import functools
import jax
import jax.numpy as jnp
from jax import lax
from jax.experimental import pallas as pl
from jax.experimental.pallas import tpu as pltpu
from jax.sharding import PartitionSpec as P

GROUPS = 32
EPS = 1e-6
C = 256
S = 16
LANES = 128
TAPS = 27
BF = jnp.bfloat16
F32 = jnp.float32
PAIR = (0, 1)
BOTH = [(slice(None, LANES)), (slice(LANES, None))]
MESH = pl.DeviceIdType.MESH
SMEM = pl.BlockSpec(memory_space=pltpu.SMEM)
VMEM = pl.BlockSpec(memory_space=pltpu.VMEM)
PARAMS = pltpu.CompilerParams(vmem_limit_bytes=58 * 2**20)


def sds(*shape, dtype=BF):
    return jax.ShapeDtypeStruct(shape, dtype)


def whole(*shape, lead=0):
    index = (lead,) + (0,) * (len(shape) - 1)
    return pl.BlockSpec(shape, lambda t: index, pipeline_mode=pl.Buffered(1))


def cost(flops, nbytes):
    return pl.CostEstimate(flops=flops, bytes_accessed=nbytes, transcendentals=0)


def silu(v):
    return v / (1.0 + jnp.exp(-v))


def sublane():
    return lax.broadcasted_iota(jnp.int32, (S, C), 0)


def shifted(v, down):
    edge, by = (0, 1) if down else (S - 1, S - 1)
    return jnp.where(sublane() == edge, 0.0, pltpu.roll(v, by, 0)).astype(BF)


def spread(mxu_items, vpu_items, lead):
    n, m = len(mxu_items), len(vpu_items)
    done = 0
    for k, item in enumerate(mxu_items):
        item()
        want = 0 if k < lead else -(-m * (k - lead + 1) // (n - lead))
        for go in vpu_items[done:want]:
            go()
        done = max(done, want)
    for go in vpu_items[done:]:
        go()


def add_sums(st_ref, frame, rows):
    v = rows.astype(F32).reshape(-1, 8, C)
    st_ref[frame, 0] += jnp.sum(v, axis=0)
    st_ref[frame, 1] += jnp.sum(v * v, axis=0)


def conv_body(H, J, R, wi, nf, nsub, has_res, natural, aliased, *refs):
    it = iter(refs)
    first_ref, gn_ref, b_ref = (next(it) for _ in range(3))
    frames = [next(it) for _ in range(nf)]
    w_ref = next(it)
    res_ref = next(it) if has_res else None
    if aliased:
        next(it)
    out_ref = next(it)
    st_ref = None if natural else next(it)
    xs = next(it)
    nat = next(it) if natural else None
    HR = (5 - nf) * R
    nblk = H // (2 * HR)
    last = nblk + 1
    HP = H + 2 + 4 * HR
    PT = 4
    NP = J // PT
    of = lambda q: q * (nf - 3)
    orow = lambda q, r: r + q * R * (4 - nf)

    def half_steps(t, u, accA, accB, dum):
        base = u * 2 * HR

        def act_item(f, r, j):
            def go():
                v = frames[f][0, base + r, j].astype(F32)
                if f < nsub:
                    v = jnp.where(first_ref[0] == 1, frames[nsub][0, base + r, j].astype(F32), v)
                xn = ((v - gn_ref[0:1, :]) * gn_ref[1:2, :] + gn_ref[2:3, :]).astype(BF).astype(F32)
                s = jnp.where(t < nblk, silu(xn), 0.0)
                dst = f * HP + t * (2 * HR) + r + 1
                xs[dst, j + 1] = s.astype(BF)
                if j == 0:
                    xs[dst, J + 1] = shifted(s, False)
                if j == J - 1:
                    xs[dst, 0] = shifted(s, True)
            return go

        def act_items(half):
            return [act_item(f, half * HR + r, j) for r in range(HR) for f in range(nf) for j in range(J)]

        def act_only():
            def go(r, _):
                for f in range(nf):
                    for j in range(J):
                        act_item(f, r, j)()
                return 0
            lax.fori_loop(0, jnp.where(t == 0, 2 * HR, HR), go, 0)

        def pop_item(acc, q, half, r, piece):
            def go():
                row = base + half * HR + orow(q, r)
                tiles = pl.ds(piece * PT, PT)
                v = pltpu.matmul_pop(acc) + b_ref[wi:wi + 1, :]
                ob = v.astype(BF)
                if has_res:
                    h = ob.astype(F32) + res_ref[of(q), row, tiles].astype(F32).reshape(PT * S, C)
                    ob = h.astype(BF)
                if natural:
                    for k in range(PT):
                        for part, cols in zip(PAIR, BOTH):
                            nat[r, q, part, pl.ds(piece * PT + k, S, stride=J), :] = h[k * S:(k + 1) * S, cols]
                    if piece == NP - 1:
                        for part, cols in zip(PAIR, BOTH):
                            out_ref[of(q), row, :, cols] = nat[r, q, part].astype(BF)
                else:
                    out_ref[of(q), row, tiles] = ob.reshape(PT, S, C)
                    add_sums(st_ref, of(q), ob)
            return go

        def pops(accs, half):
            return [pop_item(accs[q][r][p], q, half, r, p) for r in range(R) for q in PAIR for p in range(NP)]

        def mxu_item(accs, y0, n, r, p, half):
            kt, kh, kw = n // 9, n // 3 % 3, n % 3
            reg = (n + half) % 2
            lead = r == 0 and p == 0

            def go():
                for q in PAIR:
                    lhs = xs[(of(q) + kt) * HP + y0 + orow(q, r) + kh, pl.ds(kw + p * PT, PT)].reshape(PT * S, C)
                    pltpu.matmul_acc_lhs(accs[q][r][p], lhs, load_staged_rhs=reg if lead else None)
                if lead:
                    nxt = w_ref[0, (n + 1) % TAPS]
                    for q in PAIR:
                        pltpu.matmul_push_rhs(nxt, staging_register=1 - reg, mxu_index=q)
            return go

        def mxu_items(accs, y0, half):
            return [mxu_item(accs, y0, n, r, p, half) for n in range(TAPS) for r in range(R) for p in range(NP)]

        def dummy():
            for q in PAIR:
                pltpu.matmul_acc_lhs(dum[q], jnp.zeros((S, C), BF), load_staged_rhs=1)
                pltpu.matmul_pop(dum[q])

        @pl.when(t == 0)
        def _():
            for accs in (accA, accB):
                for q in PAIR:
                    for a in sum(accs[q], []):
                        pltpu.matmul_pop(a)
            for f in range(nf):
                xs[f * HP] = jnp.zeros((J + 2, S, C), BF)

        if not natural:
            @pl.when(t == 2)
            def _():
                st_ref[...] = jnp.zeros_like(st_ref)

        @pl.when(t < 2)
        def _():
            act_only()

        @pl.when(t >= 2)
        def _():
            spread(mxu_items(accA, (t - 2) * (2 * HR) + HR, 0), pops(accB, 0) + act_items(0), 4)

        @pl.when(t == 0)
        def _():
            dummy()
            for q in PAIR:
                pltpu.matmul_push_rhs(w_ref[0, 0], staging_register=1, mxu_index=q)

        @pl.when((t >= 1) & (t < last))
        def _():
            spread(mxu_items(accB, (t - 1) * (2 * HR), 1), pops(accA, 1) + act_items(1), 4)

        @pl.when(t == last)
        def _():
            dummy()
            for g in pops(accA, 1):
                g()

    def body(*accs):
        def step(u, _):
            half_steps(2 * pl.program_id(0) + u, u, *accs)
            return 0
        lax.fori_loop(0, 2, step, 0)

    acc = lambda q: [[pltpu.ACC(q)((PT * S, C), F32) for _ in range(NP)] for _ in range(R)]
    pl.run_scoped(body, [acc(0), acc(1)], [acc(0), acc(1)], [pltpu.ACC(q)((S, C), F32) for q in PAIR])


def conv(frames, w27, b, gn, first, wi, nsub=0, res=None, natural=False, ybuf=None):
    nf, nout = len(frames), len(frames) - 2
    _, H, J, _, _ = frames[0][0].shape
    R = 2
    rows = 4 * R * (5 - nf)
    nst = H // rows
    HP = H + 2 + rows
    outi = lambda t: jnp.maximum(t - 1, 0)
    late = pl.BlockSpec((nout, rows, J, S, C), lambda t: (0, outi(t), 0, 0, 0))
    now = lambda k: pl.BlockSpec((1, rows, J, S, C), lambda t: (k, jnp.minimum(t, nst - 1), 0, 0, 0))
    in_specs = [SMEM, whole(8, C), whole(5, C)] + [now(k) for _, k in frames] + [whole(1, TAPS, C, C, lead=wi)]
    args = [first, gn, b] + [a for a, _ in frames] + [w27]
    scratch = [pltpu.VMEM((nf * HP, J + 2, S, C), BF)]
    if res is not None:
        in_specs.append(late)
        args.append(res)
    if natural:
        fi = 1 if ybuf is None else 0
        if ybuf is not None:
            in_specs.append(pl.BlockSpec(memory_space=pl.ANY))
            args.append(ybuf)
        oshape, ospec = sds(2 * nout, H, J * S, C), pl.BlockSpec((nout, rows, J * S, C), lambda t: (fi, outi(t), 0, 0))
        scratch.append(pltpu.VMEM((R, 2, 2, J * S, LANES), F32))
    else:
        oshape, ospec = [sds(nout, H, J, S, C), sds(nout, 2, 8, C, dtype=F32)], [late, whole(nout, 2, 8, C)]
    return pl.pallas_call(
        functools.partial(conv_body, H, J, R, wi, nf, nsub, res is not None, natural, ybuf is not None),
        grid=(nst + 1,),
        in_specs=in_specs,
        out_specs=ospec,
        out_shape=oshape,
        input_output_aliases={} if ybuf is None else {len(args) - 1: 0},
        scratch_shapes=scratch,
        compiler_params=PARAMS,
        cost_estimate=cost(2 * nout * H * J * S * TAPS * C * C, 6 * nout * H * J * S * C),
        name=f"conv{wi}_{nout}{nsub}" + ("n" if natural else "t"),
    )(*args)


HU, JU, PADR, HPU, NS = 32, 4, 4, 40, 3
KINDS = [(tt, hh, ww) for tt in PAIR for hh in PAIR for ww in PAIR]
SEQ = [(n, kt, kh, kw) for n, kind in enumerate(KINDS)
       for kt in range(kind[0], 3 - kind[0], 2) for kh in range(kind[1], 3 - kind[1], 2) for kw in range(kind[2], 3 - kind[2], 2)]


def up_body(from_halo, first_ref, b_ref, xa_ref, xb_ref, w_ref, u_ref, st_ref, xs, es):
    t = pl.program_id(0)
    last = HU // 4 + 1
    slots = [lax.rem(t + k, NS) for k in range(NS)]

    def fill(f, src):
        def go(r, _):
            row = f * HPU + PADR + r
            xs[row, 1:JU + 1] = src[0, r]
            xs[row, JU + 1] = shifted(src[0, r, 0].astype(F32), False)
            xs[row, 0] = shifted(src[0, r, JU - 1].astype(F32), True)
            return 0
        lax.fori_loop(0, HU, go, 0)

    def mxu_items(accE, accF):
        def tiles_of(n):
            ww = KINDS[n][2]
            return (accF, JU, JU + 1) if ww else (accE[n // 2 % 2], JU + 1, 0)

        def push(k):
            w = w_ref[0, SEQ[k][1] * 9 + SEQ[k][2] * 3 + SEQ[k][3]]
            for q in PAIR:
                pltpu.matmul_push_rhs(w, staging_register=k % 2, mxu_index=q)

        def acc_item(k):
            n, kt, kh, kw = SEQ[k]
            tt, hh, ww = KINDS[n]
            refs, nt, _ = tiles_of(n)
            frames = PAIR if tt else (kt // 2,)

            def go():
                if k == 0:
                    push(0)
                load = k % 2
                for f in frames:
                    for i in PAIR:
                        for q in PAIR:
                            row = 4 * t - 4 + 2 * q + i + (kh // 2 if hh == 0 else 0) + PADR
                            lhs = xs[f * HPU + row, pl.ds((kw + 1) // 2, nt)].reshape(nt * S, C)
                            pltpu.matmul_acc_lhs(refs[q][tt * f * 2 + i], lhs, load_staged_rhs=load)
                        load = None
                    if f == frames[0] and k + 1 < TAPS:
                        push(k + 1)
            return go

        def pop_item(n):
            tt, hh, ww = KINDS[n]
            refs, nt, off = tiles_of(n)

            def go():
                for ai in range(tt + 1):
                    for i in PAIR:
                        for q in PAIR:
                            es[slots[0], q, tt + ai, hh, i, off:off + nt] = pltpu.matmul_pop(refs[q][2 * ai + i]).reshape(nt, S, C)
            return go

        items = []
        for k, (n, *_) in enumerate(SEQ):
            items.append(acc_item(k))
            if n and SEQ[k - 1][0] != n:
                items.append(pop_item(n - 1))
        return items + [pop_item(len(KINDS) - 1)]

    def combine_item(q, half):
        cols = BOTH[half]

        def sums(slot, qq, hh, i, w):
            e, f0, f1 = (es[slot, qq, k, hh, i, w, :, cols] for k in range(3))
            return e + f0, e + f1

        def rows_of(w):
            e = []
            for k in range(3):
                d = 2 * q + k - 1
                e.append(sums(slots[1], 1, 0, 1, w) if d < 0 else sums(slots[2], d // 2, 0, d % 2, w))
            f = [sums(slots[2], q, 1, i, w) for i in PAIR]
            return [[e[i + a][p] + f[i][p] for p in PAIR] for i in PAIR for a in PAIR]

        def go():
            bias = b_ref[2:3, cols]
            left = rows_of(0)
            tot = [[jnp.zeros((8, LANES), F32) for _ in PAIR] for _ in PAIR]
            for j in range(JU):
                mid, right = rows_of(JU + 1 + j), rows_of(j + 1)
                for o in range(4):
                    for p in PAIR:
                        m = mid[o][p] + bias
                        for bc, side in zip(PAIR, (left, right)):
                            ob = (side[o][p] + m).astype(BF)
                            u_ref[p, 4 * q + o, 2 * j + bc, :, cols] = ob
                            v = ob.astype(F32).reshape(2, 8, LANES)
                            tot[p][0] += jnp.sum(v, axis=0)
                            tot[p][1] += jnp.sum(v * v, axis=0)
                left = right
            for p in PAIR:
                for z in PAIR:
                    st_ref[p, z, :, cols] += tot[p][z]
        return go

    def body(accE, accF):
        combine = [combine_item(q, half) for q in PAIR for half in PAIR]

        @pl.when(t == 0)
        def _():
            for q in PAIR:
                for a in accE[0][q] + accE[1][q] + accF[q]:
                    pltpu.matmul_pop(a)
            for f in PAIR:
                for r in list(range(PADR)) + list(range(PADR + HU, HPU)):
                    xs[f * HPU + r] = jnp.zeros((JU + 2, S, C), BF)
            fill(1, xb_ref)
            if from_halo:
                @pl.when(first_ref[0] == 1)
                def _():
                    fill(0, xb_ref)

                @pl.when(first_ref[0] == 0)
                def _():
                    fill(0, xa_ref)
            else:
                fill(0, xa_ref)

        @pl.when(t == 2)
        def _():
            st_ref[...] = jnp.zeros_like(st_ref)

        @pl.when(t < last)
        def _():
            spread(mxu_items(accE, accF), combine, 2)

        @pl.when(t == last)
        def _():
            for g in combine:
                g()

    refs = lambda tiles: [[pltpu.ACC(q)((tiles * S, C), F32) for _ in range(4)] for q in PAIR]
    pl.run_scoped(body, [refs(JU + 1), refs(JU + 1)], refs(JU))


def up_conv(xa, xb, w27, b, first, from_halo):
    frame = (1, HU, JU, S, C)
    return pl.pallas_call(
        functools.partial(up_body, from_halo),
        grid=(HU // 4 + 2,),
        in_specs=[SMEM, whole(5, C), whole(*frame), whole(*frame), whole(1, TAPS, C, C, lead=2)],
        out_specs=[pl.BlockSpec((2, 8, 2 * JU, S, C), lambda t: (0, jnp.clip(t - 2, 0, HU // 4 - 1), 0, 0, 0)), whole(2, 2, 8, C)],
        out_shape=[sds(2, 2 * HU, 2 * JU, S, C), sds(2, 2, 8, C, dtype=F32)],
        scratch_shapes=[pltpu.VMEM((2 * HPU, JU + 2, S, C), BF), pltpu.VMEM((NS, 2, 3, 2, 2, 2 * JU + 1, S, C), F32)],
        compiler_params=PARAMS,
        cost_estimate=cost(2 * xb.size * TAPS * C, 10 * xb.size),
        name="up" + ("h" if from_halo else ""),
    )(first, b, xa, xb, w27)


def prep_body(z_ref, z0_ref, z1_ref, st_ref, tmp):
    @pl.when(pl.program_id(0) == 0)
    def _():
        st_ref[...] = jnp.zeros_like(st_ref)

    for f in PAIR:
        for r in range(z_ref.shape[1]):
            v = z_ref[f, r].astype(F32)
            add_sums(st_ref, f, v)
            for half, cols in zip(PAIR, BOTH):
                tmp[f, r, half] = v[:, cols]
        for r in range(z_ref.shape[1]):
            for j in range(JU):
                for half, cols in zip(PAIR, BOTH):
                    (z0_ref, z1_ref)[f][0, r, j, :, cols] = tmp[f, r, half, pl.ds(j, S, stride=JU), :].astype(BF)


def prep(z):
    rows, width = 8, JU * S
    return pl.pallas_call(
        prep_body,
        grid=(HU // rows,),
        in_specs=[pl.BlockSpec((2, rows, width, C), lambda t: (0, t, 0, 0))],
        out_specs=[pl.BlockSpec((1, rows, JU, S, C), lambda t: (0, t, 0, 0, 0))] * 2 + [whole(2, 2, 8, C)],
        out_shape=[sds(1, HU, JU, S, C)] * 2 + [sds(2, 2, 8, C, dtype=F32)],
        scratch_shapes=[pltpu.VMEM((2, rows, 2, width, LANES), F32)],
        compiler_params=PARAMS,
        cost_estimate=cost(8 * z.size, 4 * z.size),
        name="prep",
    )(z)


def stats_body(n, gi, cnt, drop, *refs):
    sts, (gamma_ref, beta_ref, gn_ref, mine, chip, recv, send_sem, recv_sem) = refs[:n], refs[n:]
    me = lax.axis_index("t")
    mate = me + 1 - 2 * lax.rem(me, 2)
    barrier = pltpu.get_barrier_semaphore()
    for d in range(1, 4):
        pl.semaphore_signal(barrier, inc=1, device_id={"t": lax.rem(me + d, 4)}, device_id_type=MESH)
    keep = jnp.where(me == 0, 0.0, 1.0) if drop else 1.0
    for z in PAIR:
        tot = None
        for st in sts:
            for f in range(st.shape[0]):
                v = st[f, z]
                if drop and st is sts[0] and f == 0:
                    v = v * keep
                tot = v if tot is None else tot + v
        mine[z] = tot
    pl.semaphore_wait(barrier, 3)

    def copy(src, slot, dev, sem):
        return pltpu.make_async_remote_copy(
            src_ref=src, dst_ref=recv.at[slot], send_sem=send_sem.at[sem], recv_sem=recv_sem.at[slot],
            device_id={"t": dev}, device_id_type=MESH)

    swap = copy(mine, 0, mate, 0)
    swap.start()
    swap.wait()
    chip[...] = mine[...] + recv[0]

    @pl.when(me == 0)
    def _():
        out = [copy(chip, 1, 2, 1), copy(chip, 1, 3, 2)]
        for c in out:
            c.start()
        for c in out:
            c.wait_send()

    @pl.when(me >= 2)
    def _():
        c = copy(chip, 1, me - 2, 1)
        c.start()
        c.wait_send()

    copy(chip, 1, mate, 1).wait_recv()
    both = jnp.sum(chip[...] + recv[1], axis=1)
    s = jnp.concatenate([both, jnp.zeros((6, C), F32)], axis=0)
    lane = lax.broadcasted_iota(jnp.int32, s.shape, 1)
    for d in (1, 2, 4):
        s = s + jnp.where((lane & d) == 0, pltpu.roll(s, C - d, 1), pltpu.roll(s, d, 1))
    mean = s[0:1] / cnt
    inv = lax.rsqrt(s[1:2] / cnt - mean * mean + EPS)
    gn_ref[...] = jnp.zeros_like(gn_ref)
    gn_ref[0:1, :] = mean
    gn_ref[1:2, :] = inv * gamma_ref[gi:gi + 1, :]
    gn_ref[2:3, :] = beta_ref[gi:gi + 1, :]


def stats(sts, gamma, beta, gi, cnt, drop=False):
    part = pltpu.VMEM((2, 8, C), F32)
    return pl.pallas_call(
        functools.partial(stats_body, len(sts), gi, float(cnt), drop),
        in_specs=[VMEM] * (len(sts) + 2),
        out_specs=VMEM,
        out_shape=sds(8, C, dtype=F32),
        scratch_shapes=[part, part, pltpu.VMEM((2, 2, 8, C), F32), pltpu.SemaphoreType.DMA((3,)), pltpu.SemaphoreType.DMA((2,))],
        compiler_params=pltpu.CompilerParams(collective_id=gi, has_side_effects=True),
        name=f"stats_{gi}",
    )(*sts, gamma, beta)


def solution(mesh):
    nt = mesh.shape['t']
    send = lambda x: lax.ppermute(x, 't', [(i, i + 1) for i in range(nt - 1)])

    def local(z, w, b, gamma, beta):
        first = (lax.axis_index('t') == 0).astype(jnp.int32).reshape(1)
        w27 = w.reshape(-1, TAPS, C, C)
        cnt1 = nt * z.size // GROUPS
        cnt2 = (2 * 2 * nt - 1) * 4 * z.size // (2 * GROUPS)
        run = lambda frames, gn, wi, **kw: conv(frames, w27, b, gn, first, wi, **kw)
        tie = lambda x, y: lax.optimization_barrier((x, y))[0]
        z0, z1, st = prep(z)
        zb = send(z1)
        za = send(tie(z0, zb))
        gn = stats([st], gamma, beta, 0, cnt1)
        h1, st1 = run([(zb, 0), (z0, 0), (z1, 0)], gn, 0, nsub=1)
        hb = send(h1)
        h0, st0 = run([(za, 0), (zb, 0), (z0, 0)], gn, 0, nsub=2)
        ha = send(tie(h0, hb))
        gn = stats([st0, st1], gamma, beta, 1, cnt1)
        x1, _ = run([(hb, 0), (h0, 0), (h1, 0)], gn, 1, nsub=1, res=z1)
        xh = send(x1)
        x0, _ = run([(ha, 0), (hb, 0), (h0, 0)], gn, 1, nsub=2, res=z0)
        u23, st23 = up_conv(x0, x1, w27, b, first, False)
        uh = send(tie(u23, xh))
        u01, st01 = up_conv(xh, x0, w27, b, first, True)
        gn = stats([st01, st23], gamma, beta, 2, cnt2, drop=True)
        pair = lambda lo, hi: [(lo, 0), (lo, 1), (hi, 0), (hi, 1)]
        h23, st23 = run(pair(u01, u23), gn, 3)
        hh = send(h23)
        h01, st01 = run(pair(uh, u01), gn, 3, nsub=2)
        gn = stats([st01, st23], gamma, beta, 3, cnt2, drop=True)
        y = run(pair(h01, h23), gn, 4, res=u23, natural=True)
        return run(pair(hh, h01), gn, 4, nsub=2, res=u01, natural=True, ybuf=y)

    spec = P(('batch', 't'))
    return jax.shard_map(local, mesh=mesh, in_specs=(spec, P(), P(), P(), P()), out_specs=spec, check_vma=False)
```

```python
import functools
import jax
import jax.numpy as jnp
from jax import lax
from jax.experimental import pallas as pl
from jax.experimental.pallas import tpu as pltpu
from jax.sharding import PartitionSpec as P


GROUPS = 32
EPS = 1e-6
C = 256
S = 16
LANES = 128
TAPS = 27
BF = jnp.bfloat16
F32 = jnp.float32
PAIR = (0, 1)
BOTH = [(slice(None, LANES)), (slice(LANES, None))]
MESH = pl.DeviceIdType.MESH
SMEM = pl.BlockSpec(memory_space=pltpu.SMEM)
VMEM = pl.BlockSpec(memory_space=pltpu.VMEM)
ANY = pl.BlockSpec(memory_space=pl.ANY)
WEIGHTS = [pltpu.VMEM((TAPS, C, C), BF), pltpu.SemaphoreType.DMA]


def params(mib):
    return pltpu.CompilerParams(vmem_limit_bytes=mib * 2**20)


def sds(*shape, dtype=BF):
    return jax.ShapeDtypeStruct(shape, dtype)


def whole(*shape, lead=0):
    index = (lead,) + (0,) * (len(shape) - 1)
    return pl.BlockSpec(shape, lambda t: index, pipeline_mode=pl.Buffered(1))


def cost(flops, nbytes):
    return pl.CostEstimate(flops=flops, bytes_accessed=nbytes, transcendentals=0)


def silu(v):
    return v / (1.0 + jnp.exp(-v))


def sublane():
    return lax.broadcasted_iota(jnp.int32, (S, C), 0)


def shifted(v, down):
    edge, by = (0, 1) if down else (S - 1, S - 1)
    return jnp.where(sublane() == edge, 0.0, pltpu.roll(v, by, 0)).astype(BF)


def spread(mxu_items, vpu_items, lead):
    n, m = len(mxu_items), len(vpu_items)
    done = 0
    for k, item in enumerate(mxu_items):
        item()
        want = 0 if k < lead else -(-m * (k - lead + 1) // (n - lead))
        for go in vpu_items[done:want]:
            go()
        done = max(done, want)
    for go in vpu_items[done:]:
        go()


def add_sums(st_ref, frame, rows):
    v = rows.astype(F32).reshape(-1, 8, C)
    st_ref[frame, 0] += jnp.sum(v, axis=0)
    st_ref[frame, 1] += jnp.sum(v * v, axis=0)


def conv_body(H, J, R, wi, nf, nsub, has_res, natural, aliased, *refs):
    it = iter(refs)
    first_ref, gn_ref, b_ref = (next(it) for _ in range(3))
    frames = [next(it) for _ in range(nf)]
    w_hbm = next(it)
    res = [next(it) for _ in range(nf - 2)] if has_res else None
    if aliased:
        next(it)
    out_ref = next(it)
    st_ref = None if natural else next(it)
    xs, w_ref, sem = (next(it) for _ in range(3))
    nat = next(it) if natural else None
    weights = pltpu.make_async_copy(w_hbm.at[wi], w_ref, sem)
    HR = (5 - nf) * R
    nblk = H // (2 * HR)
    last = nblk + 1
    HP = H + 2 + 4 * HR
    PT = 4
    NP = J // PT
    of = lambda q: q * (nf - 3)
    orow = lambda q, r: r + q * R * (4 - nf)

    def half_steps(t, u, accA, accB, dum):
        base = u * 2 * HR

        def act_item(f, r, j):
            def go():
                v = frames[f][0, base + r, j].astype(F32)
                if f < nsub:
                    v = jnp.where(first_ref[0] == 1, frames[nsub][0, base + r, j].astype(F32), v)
                xn = ((v - gn_ref[0:1, :]) * gn_ref[1:2, :] + gn_ref[2:3, :]).astype(BF).astype(F32)
                s = jnp.where(t < nblk, silu(xn), 0.0)
                dst = f * HP + t * (2 * HR) + r + 1
                xs[dst, j + 1] = s.astype(BF)
                if j == 0:
                    xs[dst, J + 1] = shifted(s, False)
                if j == J - 1:
                    xs[dst, 0] = shifted(s, True)

            return go

        def act_items(half):
            return [act_item(f, half * HR + r, j) for r in range(HR) for f in range(nf) for j in range(J)]

        def act_only():
            def go(r, _):
                for f in range(nf):
                    for j in range(J):
                        act_item(f, r, j)()
                return 0

            lax.fori_loop(0, jnp.where(t == 0, 2 * HR, HR), go, 0)

        def pop_item(acc, q, half, r, piece):
            def go():
                row = base + half * HR + orow(q, r)
                tiles = pl.ds(piece * PT, PT)
                v = pltpu.matmul_pop(acc) + b_ref[wi:wi + 1, :]
                ob = v.astype(BF)
                if has_res:
                    h = ob.astype(F32) + res[of(q)][0, row, tiles].astype(F32).reshape(PT * S, C)
                    ob = h.astype(BF)
                if natural:
                    for k in range(PT):
                        for part, cols in zip(PAIR, BOTH):
                            nat[r, q, part, pl.ds(piece * PT + k, S, stride=J), :] = h[k * S:(k + 1) * S, cols]
                    if piece == NP - 1:
                        for part, cols in zip(PAIR, BOTH):
                            out_ref[of(q), row, :, cols] = nat[r, q, part].astype(BF)
                else:
                    out_ref[of(q), row, tiles] = ob.reshape(PT, S, C)
                    add_sums(st_ref, of(q), ob)

            return go

        def pops(accs, half):
            return [pop_item(accs[q][r][p], q, half, r, p) for r in range(R) for q in PAIR for p in range(NP)]

        def mxu_item(accs, y0, n, r, p, half):
            kt, kh, kw = n // 9, n // 3 % 3, n % 3
            reg = (n + half) % 2
            lead = r == 0 and p == 0

            def go():
                for q in PAIR:
                    lhs = xs[(of(q) + kt) * HP + y0 + orow(q, r) + kh, pl.ds(kw + p * PT, PT)].reshape(PT * S, C)
                    pltpu.matmul_acc_lhs(accs[q][r][p], lhs, load_staged_rhs=reg if lead else None)
                if lead:
                    nxt = w_ref[(n + 1) % TAPS]
                    for q in PAIR:
                        pltpu.matmul_push_rhs(nxt, staging_register=1 - reg, mxu_index=q)

            return go

        def mxu_items(accs, y0, half):
            return [mxu_item(accs, y0, n, r, p, half) for n in range(TAPS) for r in range(R) for p in range(NP)]

        def dummy():
            for q in PAIR:
                pltpu.matmul_acc_lhs(dum[q], jnp.zeros((S, C), BF), load_staged_rhs=1)
                pltpu.matmul_pop(dum[q])

        @pl.when(t == 0)
        def _():
            weights.start()
            for accs in (accA, accB):
                for q in PAIR:
                    for a in sum(accs[q], []):
                        pltpu.matmul_pop(a)
            for f in range(nf):
                xs[f * HP] = jnp.zeros((J + 2, S, C), BF)

        if not natural:
            @pl.when(t == 2)
            def _():
                st_ref[...] = jnp.zeros_like(st_ref)

        @pl.when(t < 2)
        def _():
            act_only()

        @pl.when(t >= 2)
        def _():
            spread(mxu_items(accA, (t - 2) * (2 * HR) + HR, 0), pops(accB, 0) + act_items(0), 0)

        @pl.when(t == 0)
        def _():
            dummy()
            weights.wait()
            for q in PAIR:
                pltpu.matmul_push_rhs(w_ref[0], staging_register=1, mxu_index=q)

        @pl.when((t >= 1) & (t < last))
        def _():
            spread(mxu_items(accB, (t - 1) * (2 * HR), 1), pops(accA, 1) + act_items(1), 0)

        @pl.when(t == last)
        def _():
            dummy()
            for g in pops(accA, 1):
                g()

    def body(*accs):
        def step(u, _):
            half_steps(2 * pl.program_id(0) + u, u, *accs)
            return 0

        lax.fori_loop(0, 2, step, 0)

    acc = lambda q: [[pltpu.ACC(q)((PT * S, C), F32) for _ in range(NP)] for _ in range(R)]
    pl.run_scoped(body, [acc(0), acc(1)], [acc(0), acc(1)], [pltpu.ACC(q)((S, C), F32) for q in PAIR])


def conv(frames, w27, b, gn, first, wi, nsub=0, res=None, natural=False, ybuf=None):
    nf, nout = len(frames), len(frames) - 2
    _, H, J, _, _ = frames[0][0].shape
    R = 2
    rows = 4 * R * (5 - nf)
    nst = H // rows
    HP = H + 2 + rows
    outi = lambda t: jnp.maximum(t - 1, 0)
    late = pl.BlockSpec((nout, rows, J, S, C), lambda t: (0, outi(t), 0, 0, 0))
    now = lambda k: pl.BlockSpec((1, rows, J, S, C), lambda t: (k, jnp.minimum(t, nst - 1), 0, 0, 0))
    in_specs = [SMEM, whole(8, C), whole(5, C)] + [now(k) for _, k in frames] + [ANY]
    args = [first, gn, b] + [a for a, _ in frames] + [w27]
    scratch = [pltpu.VMEM((nf * HP, J + 2, S, C), BF)] + WEIGHTS
    for a, k in res or ():
        in_specs.append(pl.BlockSpec((1, rows, J, S, C), lambda t, k=k: (k, outi(t), 0, 0, 0)))
        args.append(a)
    if natural:
        fi = 1 if ybuf is None else 0
        if ybuf is not None:
            in_specs.append(ANY)
            args.append(ybuf)
        oshape, ospec = sds(2 * nout, H, J * S, C), pl.BlockSpec((nout, rows, J * S, C), lambda t: (fi, outi(t), 0, 0))
        scratch.append(pltpu.VMEM((R, 2, 2, J * S, LANES), F32))
    else:
        oshape, ospec = [sds(nout, H, J, S, C), sds(nout, 2, 8, C, dtype=F32)], [late, whole(nout, 2, 8, C)]
    return pl.pallas_call(
        functools.partial(conv_body, H, J, R, wi, nf, nsub, res is not None, natural, ybuf is not None),
        grid=(nst + 1,),
        in_specs=in_specs,
        out_specs=ospec,
        out_shape=oshape,
        input_output_aliases={} if ybuf is None else {len(args) - 1: 0},
        scratch_shapes=scratch,
        compiler_params=params(46 if H == HU else 61),
        cost_estimate=cost(2 * nout * H * J * S * TAPS * C * C, 6 * nout * H * J * S * C),
    )(*args)


HU, JU, PADR, HPU, NS = 32, 4, 4, 40, 3
KINDS = [(tt, hh, ww) for tt in PAIR for hh in PAIR for ww in PAIR]
SEQ = [(n, kt, kh, kw) for n, kind in enumerate(KINDS)
       for kt in range(kind[0], 3 - kind[0], 2) for kh in range(kind[1], 3 - kind[1], 2) for kw in range(kind[2], 3 - kind[2], 2)]


def up_body(from_halo, first_ref, b_ref, xa_ref, xb_ref, w_hbm, u_ref, st_ref, xs, es, w_ref, sem):
    t = pl.program_id(0)
    last = HU // 4 + 1
    slots = [lax.rem(t + k, NS) for k in range(NS)]
    weights = pltpu.make_async_copy(w_hbm.at[2], w_ref, sem)

    def fill(f, src):
        def go(i, _):
            for r in range(8):
                r = i * 8 + r
                row = f * HPU + PADR + r
                xs[row, 1:JU + 1] = src[0, r]
                xs[row, JU + 1] = shifted(src[0, r, 0].astype(F32), False)
                xs[row, 0] = shifted(src[0, r, JU - 1].astype(F32), True)
            return 0

        lax.fori_loop(0, HU // 8, go, 0)

    def mxu_items(accE, accF):
        def tiles_of(n):
            ww = KINDS[n][2]
            return (accF, JU, JU + 1) if ww else (accE[n // 2 % 2], JU + 1, 0)

        def push(k):
            w = w_ref[SEQ[k][1] * 9 + SEQ[k][2] * 3 + SEQ[k][3]]
            for q in PAIR:
                pltpu.matmul_push_rhs(w, staging_register=k % 2, mxu_index=q)

        def acc_item(k):
            n, kt, kh, kw = SEQ[k]
            tt, hh, _ = KINDS[n]
            refs, nt, _ = tiles_of(n)
            frames = PAIR if tt else (kt // 2,)

            def go():
                if k == 0:
                    push(0)
                load = k % 2
                for f in frames:
                    for i in PAIR:
                        for q in PAIR:
                            row = 4 * t - 4 + 2 * q + i + (kh // 2 if hh == 0 else 0) + PADR
                            lhs = xs[f * HPU + row, pl.ds((kw + 1) // 2, nt)].reshape(nt * S, C)
                            pltpu.matmul_acc_lhs(refs[q][tt * f * 2 + i], lhs, load_staged_rhs=load)
                        load = None
                    if f == frames[0] and k + 1 < TAPS:
                        push(k + 1)

            return go

        def pop_item(n):
            tt, hh, _ = KINDS[n]
            refs, nt, off = tiles_of(n)

            def go():
                for ai in range(tt + 1):
                    for i in PAIR:
                        for q in PAIR:
                            es[slots[0], q, tt + ai, hh, i, off:off + nt] = pltpu.matmul_pop(refs[q][2 * ai + i]).reshape(nt, S, C)

            return go

        items = []
        for k, (n, *_) in enumerate(SEQ):
            items.append(acc_item(k))
            if n and SEQ[k - 1][0] != n:
                items.append(pop_item(n - 1))
        return items + [pop_item(len(KINDS) - 1)]

    def combine_item(q, half):
        cols = BOTH[half]

        def sums(slot, qq, hh, i, w):
            e, f0, f1 = (es[slot, qq, k, hh, i, w, :, cols] for k in range(3))
            return e + f0, e + f1

        def rows_of(w):
            e = []
            for k in range(3):
                d = 2 * q + k - 1
                e.append(sums(slots[1], 1, 0, 1, w) if d < 0 else sums(slots[2], d // 2, 0, d % 2, w))
            f = [sums(slots[2], q, 1, i, w) for i in PAIR]
            return [[e[i + a][p] + f[i][p] for p in PAIR] for i in PAIR for a in PAIR]

        def go():
            bias = b_ref[2:3, cols]
            left = rows_of(0)
            tot = [[jnp.zeros((8, LANES), F32) for _ in PAIR] for _ in PAIR]
            for j in range(JU):
                mid, right = rows_of(JU + 1 + j), rows_of(j + 1)
                for o in range(4):
                    for p in PAIR:
                        m = mid[o][p] + bias
                        for bc, side in zip(PAIR, (left, right)):
                            ob = (side[o][p] + m).astype(BF)
                            u_ref[p, 4 * q + o, 2 * j + bc, :, cols] = ob
                            v = ob.astype(F32).reshape(2, 8, LANES)
                            tot[p][0] += jnp.sum(v, axis=0)
                            tot[p][1] += jnp.sum(v * v, axis=0)
                left = right
            for p in PAIR:
                for z in PAIR:
                    st_ref[p, z, :, cols] += tot[p][z]

        return go

    def body(accE, accF):
        combine = [combine_item(q, half) for q in PAIR for half in PAIR]

        @pl.when(t == 0)
        def _():
            weights.start()
            for q in PAIR:
                for a in accE[0][q] + accE[1][q] + accF[q]:
                    pltpu.matmul_pop(a)
            for f in PAIR:
                for r in list(range(PADR)) + list(range(PADR + HU, HPU)):
                    xs[f * HPU + r] = jnp.zeros((JU + 2, S, C), BF)
            fill(1, xb_ref)
            if from_halo:
                @pl.when(first_ref[0] == 1)
                def _():
                    fill(0, xb_ref)

                @pl.when(first_ref[0] == 0)
                def _():
                    fill(0, xa_ref)
            else:
                fill(0, xa_ref)
            weights.wait()

        @pl.when(t == 2)
        def _():
            st_ref[...] = jnp.zeros_like(st_ref)

        @pl.when(t < last)
        def _():
            spread(mxu_items(accE, accF), combine, 2)

        @pl.when(t == last)
        def _():
            for g in combine:
                g()

    refs = lambda tiles: [[pltpu.ACC(q)((tiles * S, C), F32) for _ in range(4)] for q in PAIR]
    pl.run_scoped(body, [refs(JU + 1), refs(JU + 1)], refs(JU))


def up_conv(a, c, w27, b, first, from_halo):
    (xa, ka), (xb, kb) = a, c
    frame = (1, HU, JU, S, C)
    return pl.pallas_call(
        functools.partial(up_body, from_halo),
        grid=(HU // 4 + 2,),
        in_specs=[SMEM, whole(5, C), whole(*frame, lead=ka), whole(*frame, lead=kb), ANY],
        out_specs=[pl.BlockSpec((2, 8, 2 * JU, S, C), lambda t: (0, jnp.clip(t - 2, 0, HU // 4 - 1), 0, 0, 0)), whole(2, 2, 8, C)],
        out_shape=[sds(2, 2 * HU, 2 * JU, S, C), sds(2, 2, 8, C, dtype=F32)],
        scratch_shapes=[pltpu.VMEM((2 * HPU, JU + 2, S, C), BF), pltpu.VMEM((NS, 2, 3, 2, 2, 2 * JU + 1, S, C), F32)] + WEIGHTS,
        compiler_params=params(46),
        cost_estimate=cost(4 * HU * JU * S * C * TAPS * C, 10 * HU * JU * S * C),
    )(first, b, xa, xb, w27)


def prep_body(z_ref, z0_ref, z1_ref, st_ref, tmp):
    @pl.when(pl.program_id(0) == 0)
    def _():
        st_ref[...] = jnp.zeros_like(st_ref)

    for f in PAIR:
        for r in range(z_ref.shape[1]):
            v = z_ref[f, r].astype(F32)
            add_sums(st_ref, f, v)
            for half, cols in zip(PAIR, BOTH):
                tmp[f, r, half] = v[:, cols]
        for r in range(z_ref.shape[1]):
            for j in range(JU):
                for half, cols in zip(PAIR, BOTH):
                    (z0_ref, z1_ref)[f][0, r, j, :, cols] = tmp[f, r, half, pl.ds(j, S, stride=JU), :].astype(BF)


def prep(z):
    rows, width = 8, JU * S
    return pl.pallas_call(
        prep_body,
        grid=(HU // rows,),
        in_specs=[pl.BlockSpec((2, rows, width, C), lambda t: (0, t, 0, 0))],
        out_specs=[pl.BlockSpec((1, rows, JU, S, C), lambda t: (0, t, 0, 0, 0))] * 2 + [whole(2, 2, 8, C)],
        out_shape=[sds(1, HU, JU, S, C)] * 2 + [sds(2, 2, 8, C, dtype=F32)],
        scratch_shapes=[pltpu.VMEM((2, rows, 2, width, LANES), F32)],
        compiler_params=params(46),
        cost_estimate=cost(8 * z.size, 4 * z.size),
        name="prep",
    )(z)


def stats_body(n, gi, cnt, drop, *refs):
    sts, (gamma_ref, beta_ref, gn_ref, mine, chip, recv, send_sem, recv_sem) = refs[:n], refs[n:]
    me = lax.axis_index("t")
    mate = me + 1 - 2 * lax.rem(me, 2)
    barrier = pltpu.get_barrier_semaphore()
    for d in range(1, 4):
        pl.semaphore_signal(barrier, inc=1, device_id={"t": lax.rem(me + d, 4)}, device_id_type=MESH)
    keep = jnp.where(me == 0, 0.0, 1.0) if drop else 1.0
    for z in PAIR:
        tot = None
        for st in sts:
            for f in range(st.shape[0]):
                v = st[f, z]
                if drop and st is sts[0] and f == 0:
                    v = v * keep
                tot = v if tot is None else tot + v
        mine[z] = tot
    pl.semaphore_wait(barrier, 3)

    def copy(src, slot, dev, sem):
        return pltpu.make_async_remote_copy(
            src_ref=src, dst_ref=recv.at[slot], send_sem=send_sem.at[sem], recv_sem=recv_sem.at[slot],
            device_id={"t": dev}, device_id_type=MESH)

    swap = copy(mine, 0, mate, 0)
    swap.start()
    swap.wait()
    chip[...] = mine[...] + recv[0]

    @pl.when(me == 0)
    def _():
        out = [copy(chip, 1, 2, 1), copy(chip, 1, 3, 2)]
        for c in out:
            c.start()
        for c in out:
            c.wait_send()

    @pl.when(me >= 2)
    def _():
        c = copy(chip, 1, me - 2, 1)
        c.start()
        c.wait_send()

    copy(chip, 1, mate, 1).wait_recv()
    both = jnp.sum(chip[...] + recv[1], axis=1)
    s = jnp.concatenate([both, jnp.zeros((6, C), F32)], axis=0)
    lane = lax.broadcasted_iota(jnp.int32, s.shape, 1)
    for d in (1, 2, 4):
        s = s + jnp.where((lane & d) == 0, pltpu.roll(s, C - d, 1), pltpu.roll(s, d, 1))
    mean = s[0:1] / cnt
    inv = lax.rsqrt(s[1:2] / cnt - mean * mean + EPS)
    gn_ref[...] = jnp.zeros_like(gn_ref)
    gn_ref[0:1, :] = mean
    gn_ref[1:2, :] = inv * gamma_ref[gi:gi + 1, :]
    gn_ref[2:3, :] = beta_ref[gi:gi + 1, :]


def stats(sts, gamma, beta, gi, cnt, drop=False):
    part = pltpu.VMEM((2, 8, C), F32)
    return pl.pallas_call(
        functools.partial(stats_body, len(sts), gi, float(cnt), drop),
        in_specs=[VMEM] * (len(sts) + 2),
        out_specs=VMEM,
        out_shape=sds(8, C, dtype=F32),
        scratch_shapes=[part, part, pltpu.VMEM((2, 2, 8, C), F32), pltpu.SemaphoreType.DMA((3,)), pltpu.SemaphoreType.DMA((2,))],
        compiler_params=pltpu.CompilerParams(collective_id=gi, has_side_effects=True, vmem_limit_bytes=46 * 2**20),
    )(*sts, gamma, beta)


def solution(mesh):
    nt = mesh.shape['t']

    hbm = lambda x: pltpu.with_memory_space_constraint(x, pltpu.HBM)

    def send(x):
        return lax.ppermute(x, 't', [(i, i + 1) for i in range(nt - 1)])

    def local(z, w, b, gamma, beta):
        first = (lax.axis_index('t') == 0).astype(jnp.int32).reshape(1)
        w27 = w.reshape(-1, TAPS, C, C)
        cnt1 = nt * z.size // GROUPS
        cnt2 = (2 * 2 * nt - 1) * 4 * z.size // (2 * GROUPS)
        run = lambda frames, gn, wi, **kw: conv(frames, w27, b, gn, first, wi, **kw)
        z0, z1, st = prep(hbm(z))
        zb = send(z1)
        za = send(z0)
        gn = stats([st], gamma, beta, 0, cnt1)
        h1, st1 = run([(zb, 0), (z0, 0), (z1, 0)], gn, 0, nsub=1)
        hb = send(h1)
        h0, st0 = run([(za, 0), (zb, 0), (z0, 0)], gn, 0, nsub=2)
        ha = send(h0)
        gn = stats([st0, st1], gamma, beta, 1, cnt1)
        x1, _ = run([(hb, 0), (h0, 0), (h1, 0)], gn, 1, nsub=1, res=[(z1, 0)])
        xh = send(x1)
        x0, _ = run([(ha, 0), (hb, 0), (h0, 0)], gn, 1, nsub=2, res=[(z0, 0)])
        u23, st23 = up_conv((x0, 0), (x1, 0), w27, b, first, False)
        uh = send(u23)
        u01, st01 = up_conv((xh, 0), (x0, 0), w27, b, first, True)
        gn = stats([st01, st23], gamma, beta, 2, cnt2, drop=True)
        pair = lambda lo, hi: [(lo, 0), (lo, 1), (hi, 0), (hi, 1)]
        h23, st23 = run(pair(u01, u23), gn, 3)
        hh = send(h23)
        h01, st01 = run(pair(uh, u01), gn, 3, nsub=2)
        gn = stats([st01, st23], gamma, beta, 3, cnt2, drop=True)
        y = run(pair(h01, h23), gn, 4, res=[(u23, 0), (u23, 1)], natural=True)
        return run(pair(hh, h01), gn, 4, nsub=2, res=[(u01, 0), (u01, 1)], natural=True, ybuf=y)

    spec = P(('batch', 't'))

    return jax.shard_map(local, mesh=mesh, in_specs=(spec, P(), P(), P(), P()), out_specs=spec, check_vma=False)
```

```python
import functools
import jax
import jax.numpy as jnp
from jax import lax
from jax.experimental import pallas as pl
from jax.experimental.pallas import tpu as pltpu
from jax.sharding import PartitionSpec as P


GROUPS = 32
EPS = 1e-6
C = 256
S = 16
LANES = 128
TAPS = 27
BF = jnp.bfloat16
F32 = jnp.float32
PAIR = (0, 1)
BOTH = [(slice(None, LANES)), (slice(LANES, None))]
MESH = pl.DeviceIdType.MESH
SMEM = pl.BlockSpec(memory_space=pltpu.SMEM)
VMEM = pl.BlockSpec(memory_space=pltpu.VMEM)
ANY = pl.BlockSpec(memory_space=pl.ANY)
WEIGHTS = [pltpu.VMEM((TAPS, C, C), BF), pltpu.SemaphoreType.DMA]


def params(mib):
    return pltpu.CompilerParams(vmem_limit_bytes=mib * 2**20)


def sds(*shape, dtype=BF):
    return jax.ShapeDtypeStruct(shape, dtype)


def whole(*shape, lead=0):
    index = (lead,) + (0,) * (len(shape) - 1)
    return pl.BlockSpec(shape, lambda t: index, pipeline_mode=pl.Buffered(1))


def cost(flops, nbytes):
    return pl.CostEstimate(flops=flops, bytes_accessed=nbytes, transcendentals=0)


def silu(v):
    return v / (1.0 + jnp.exp(-v))


def sublane():
    return lax.broadcasted_iota(jnp.int32, (S, C), 0)


def shifted(v, down):
    edge, by = (0, 1) if down else (S - 1, S - 1)
    return jnp.where(sublane() == edge, 0.0, pltpu.roll(v, by, 0)).astype(BF)


def spread(mxu_items, vpu_items, lead):
    n, m = len(mxu_items), len(vpu_items)
    done = 0
    for k, item in enumerate(mxu_items):
        item()
        want = 0 if k < lead else -(-m * (k - lead + 1) // (n - lead))
        for go in vpu_items[done:want]:
            go()
        done = max(done, want)
    for go in vpu_items[done:]:
        go()


def add_sums(st_ref, frame, rows):
    v = rows.astype(F32).reshape(-1, 8, C)
    st_ref[frame, 0] += jnp.sum(v, axis=0)
    st_ref[frame, 1] += jnp.sum(v * v, axis=0)


def conv_body(H, J, R, wi, nf, nsub, has_res, natural, aliased, *refs):
    it = iter(refs)
    first_ref, gn_ref, b_ref = (next(it) for _ in range(3))
    frames = [next(it) for _ in range(nf)]
    w_hbm = next(it)
    res = [next(it) for _ in range(nf - 2)] if has_res else None
    if aliased:
        next(it)
    out_ref = next(it)
    st_ref = None if natural else next(it)
    xs, w_ref, sem, stash = (next(it) for _ in range(4))
    nat = next(it) if natural else None
    weights = pltpu.make_async_copy(w_hbm.at[wi], w_ref, sem)
    HR = (5 - nf) * R
    nblk = H // (2 * HR)
    last = nblk + 1
    HP = H + 2 + 4 * HR
    PT = J
    NP = J // PT
    of = lambda q: q * (nf - 3)
    orow = lambda q, r: r + q * R * (4 - nf)

    def half_steps(t, u, accA, accB, dum):
        base = u * 2 * HR

        def act_item(f, r, j):
            def go():
                v = frames[f][0, base + r, j]
                if f < nsub:
                    v = jnp.where(first_ref[0] == 1, frames[nsub][0, base + r, j], v)
                scale, shift = (jnp.where(t < nblk, gn_ref[k:k + 1, :], 0.0) for k in (1, 2))
                xn = ((v.astype(F32) - gn_ref[0:1, :]) * scale + shift).astype(BF).astype(F32)
                s = silu(xn)
                dst = f * HP + t * (2 * HR) + r + 1
                xs[dst, j + 1] = s.astype(BF)
                if j == 0:
                    xs[dst, J + 1] = shifted(s, False)
                if j == J - 1:
                    xs[dst, 0] = shifted(s, True)

            return go

        def act_items(half):
            return [act_item(f, half * HR + r, j) for r in range(HR) for f in range(nf) for j in range(J)]

        def act_only():
            def go(r, _):
                for f in range(nf):
                    for j in range(J):
                        act_item(f, r, j)()
                return 0

            lax.fori_loop(0, 2 * HR, go, 0)

        def result(acc):
            return (pltpu.matmul_pop(acc) + b_ref[wi:wi + 1, :]).astype(BF)

        def keep_item(acc, q, r, piece):
            def go():
                stash[q, r, pl.ds(piece * PT, PT)] = result(acc).reshape(PT, S, C)

            return go

        def out_item(acc, q, half, r, piece):
            def go():
                row = base + half * HR + orow(q, r)
                tiles = pl.ds(piece * PT, PT)
                ob = result(acc) if half else stash[q, r, tiles].reshape(PT * S, C)
                if has_res:
                    h = ob.astype(F32) + res[of(q)][0, row, tiles].astype(F32).reshape(PT * S, C)
                    ob = h.astype(BF)
                if natural:
                    for k in range(PT):
                        for part, cols in zip(PAIR, BOTH):
                            nat[r, q, part, pl.ds(piece * PT + k, S, stride=J), :] = h[k * S:(k + 1) * S, cols]
                    if piece == NP - 1:
                        for part, cols in zip(PAIR, BOTH):
                            out_ref[of(q), row, :, cols] = nat[r, q, part].astype(BF)
                else:
                    out_ref[of(q), row, tiles] = ob.reshape(PT, S, C)
                    add_sums(st_ref, of(q), ob)

            return go

        order = [(q, r, p) for r in range(R) for q in PAIR for p in range(NP)]
        keeps = [keep_item(accA[q][r][p], q, r, p) for q, r, p in order]
        outs = [out_item(accB[q][r][p], q, half, r, p) for half in (1, 0) for q, r, p in order]

        def mxu_item(accs, y0, n, r, p, half):
            kt, kh, kw = n // 9, n // 3 % 3, n % 3
            reg = (n + half) % 2
            lead = r == 0 and p == 0

            def go():
                for q in PAIR:
                    lhs = xs[(of(q) + kt) * HP + y0 + orow(q, r) + kh, pl.ds(kw + p * PT, PT)].reshape(PT * S, C)
                    pltpu.matmul_acc_lhs(accs[q][r][p], lhs, load_staged_rhs=reg if lead else None)
                if lead:
                    nxt = w_ref[(n + 1) % TAPS]
                    for q in PAIR:
                        pltpu.matmul_push_rhs(nxt, staging_register=1 - reg, mxu_index=q)

            return go

        def mxu_items(accs, y0, half):
            return [mxu_item(accs, y0, n, r, p, half) for n in range(TAPS) for r in range(R) for p in range(NP)]

        def dummy():
            for q in PAIR:
                pltpu.matmul_acc_lhs(dum[q], jnp.zeros((S, C), BF), load_staged_rhs=0)
                pltpu.matmul_pop(dum[q])

        @pl.when(t == 0)
        def _():
            weights.start()
            for accs in (accA, accB):
                for q in PAIR:
                    for a in sum(accs[q], []):
                        pltpu.matmul_pop(a)
            for f in range(nf):
                xs[f * HP] = jnp.zeros((J + 2, S, C), BF)

        if not natural:
            @pl.when(t == 2)
            def _():
                st_ref[...] = jnp.zeros_like(st_ref)

        @pl.when(t == 0)
        def _():
            act_only()
            dummy()
            weights.wait()
            for q in PAIR:
                pltpu.matmul_push_rhs(w_ref[0], staging_register=0, mxu_index=q)

        @pl.when((t >= 1) & (t < last))
        def _():
            spread(mxu_items(accA, (t - 1) * (2 * HR), 0), outs + act_items(0), 0)

        @pl.when((t >= 1) & (t < last))
        def _():
            spread(mxu_items(accB, (t - 1) * (2 * HR) + HR, 1), keeps + act_items(1), 0)

        @pl.when(t == last)
        def _():
            dummy()
            for g in outs:
                g()

    def body(*accs):
        def step(u, _):
            half_steps(2 * pl.program_id(0) + u, u, *accs)
            return 0

        lax.fori_loop(0, 2, step, 0)

    acc = lambda q: [[pltpu.ACC(q)((PT * S, C), F32) for _ in range(NP)] for _ in range(R)]
    pl.run_scoped(body, [acc(0), acc(1)], [acc(0), acc(1)], [pltpu.ACC(q)((S, C), F32) for q in PAIR])


def conv(frames, w27, b, gn, first, wi, nsub=0, res=None, natural=False, ybuf=None):
    nf, nout = len(frames), len(frames) - 2
    _, H, J, _, _ = frames[0][0].shape
    R = 2
    rows = 4 * R * (5 - nf)
    nst = H // rows
    HP = H + 2 + rows
    outi = lambda t: jnp.maximum(t - 1, 0)
    late = pl.BlockSpec((nout, rows, J, S, C), lambda t: (0, outi(t), 0, 0, 0))
    now = lambda k: pl.BlockSpec((1, rows, J, S, C), lambda t: (k, jnp.minimum(t, nst - 1), 0, 0, 0))
    in_specs = [SMEM, whole(8, C), whole(5, C)] + [now(k) for _, k in frames] + [ANY]
    args = [first, gn, b] + [a for a, _ in frames] + [w27]
    scratch = [pltpu.VMEM((nf * HP, J + 2, S, C), BF)] + WEIGHTS + [pltpu.VMEM((2, R, J, S, C), BF)]
    for a, k in res or ():
        in_specs.append(pl.BlockSpec((1, rows, J, S, C), lambda t, k=k: (k, outi(t), 0, 0, 0)))
        args.append(a)
    if natural:
        fi = 1 if ybuf is None else 0
        if ybuf is not None:
            in_specs.append(ANY)
            args.append(ybuf)
        oshape, ospec = sds(2 * nout, H, J * S, C), pl.BlockSpec((nout, rows, J * S, C), lambda t: (fi, outi(t), 0, 0))
        scratch.append(pltpu.VMEM((R, 2, 2, J * S, LANES), F32))
    else:
        oshape, ospec = [sds(nout, H, J, S, C), sds(nout, 2, 8, C, dtype=F32)], [late, whole(nout, 2, 8, C)]
    return pl.pallas_call(
        functools.partial(conv_body, H, J, R, wi, nf, nsub, res is not None, natural, ybuf is not None),
        grid=(nst + 1,),
        in_specs=in_specs,
        out_specs=ospec,
        out_shape=oshape,
        input_output_aliases={} if ybuf is None else {len(args) - 1: 0},
        scratch_shapes=scratch,
        compiler_params=params(46 if H == HU else 61),
        cost_estimate=cost(2 * nout * H * J * S * TAPS * C * C, 6 * nout * H * J * S * C),
    )(*args)


HU, JU, PADR, HPU, NS = 32, 4, 4, 40, 3
KINDS = [(tt, hh, ww) for tt in PAIR for hh in PAIR for ww in PAIR]
SEQ = [(n, kt, kh, kw) for n, kind in enumerate(KINDS)
       for kt in range(kind[0], 3 - kind[0], 2) for kh in range(kind[1], 3 - kind[1], 2) for kw in range(kind[2], 3 - kind[2], 2)]


def up_body(from_halo, first_ref, b_ref, xa_ref, xb_ref, w_hbm, u_ref, st_ref, xs, es, w_ref, sem):
    t = pl.program_id(0)
    last = HU // 4 + 1
    slots = [lax.rem(t + k, NS) for k in range(NS)]
    weights = pltpu.make_async_copy(w_hbm.at[2], w_ref, sem)

    def fill(f, src):
        def go(i, _):
            for r in range(8):
                r = i * 8 + r
                row = f * HPU + PADR + r
                xs[row, 1:JU + 1] = src[0, r]
                xs[row, JU + 1] = shifted(src[0, r, 0].astype(F32), False)
                xs[row, 0] = shifted(src[0, r, JU - 1].astype(F32), True)
            return 0

        lax.fori_loop(0, HU // 8, go, 0)

    def mxu_items(accE, accF):
        def tiles_of(n):
            ww = KINDS[n][2]
            return (accF, JU, JU + 1) if ww else (accE[n // 2 % 2], JU + 1, 0)

        def push(k):
            w = w_ref[SEQ[k][1] * 9 + SEQ[k][2] * 3 + SEQ[k][3]]
            for q in PAIR:
                pltpu.matmul_push_rhs(w, staging_register=k % 2, mxu_index=q)

        def acc_item(k):
            n, kt, kh, kw = SEQ[k]
            tt, hh, _ = KINDS[n]
            refs, nt, _ = tiles_of(n)
            frames = PAIR if tt else (kt // 2,)

            def go():
                if k == 0:
                    push(0)
                load = k % 2
                for f in frames:
                    for i in PAIR:
                        for q in PAIR:
                            row = 4 * t - 4 + 2 * q + i + (kh // 2 if hh == 0 else 0) + PADR
                            lhs = xs[f * HPU + row, pl.ds((kw + 1) // 2, nt)].reshape(nt * S, C)
                            pltpu.matmul_acc_lhs(refs[q][tt * f * 2 + i], lhs, load_staged_rhs=load)
                        load = None
                    if f == frames[0] and k + 1 < TAPS:
                        push(k + 1)

            return go

        def pop_item(n):
            tt, hh, _ = KINDS[n]
            refs, nt, off = tiles_of(n)

            def go():
                for ai in range(tt + 1):
                    for i in PAIR:
                        for q in PAIR:
                            es[slots[0], q, tt + ai, hh, i, off:off + nt] = pltpu.matmul_pop(refs[q][2 * ai + i]).reshape(nt, S, C)

            return go

        items = []
        for k, (n, *_) in enumerate(SEQ):
            items.append(acc_item(k))
            if n and SEQ[k - 1][0] != n:
                items.append(pop_item(n - 1))
        return items + [pop_item(len(KINDS) - 1)]

    def combine_items(q, half):
        cols = BOTH[half]

        def sums(slot, qq, hh, i, w):
            e, f0, f1 = (es[slot, qq, k, hh, i, w, :, cols] for k in range(3))
            return e + f0, e + f1

        def rows_of(w):
            e = []
            for k in range(3):
                d = 2 * q + k - 1
                e.append(sums(slots[1], 1, 0, 1, w) if d < 0 else sums(slots[2], d // 2, 0, d % 2, w))
            f = [sums(slots[2], q, 1, i, w) for i in PAIR]
            return [[e[i + a][p] + f[i][p] for p in PAIR] for i in PAIR for a in PAIR]

        state = {}

        def start():
            state["left"] = rows_of(0)
            state["tot"] = [[jnp.zeros((8, LANES), F32) for _ in PAIR] for _ in PAIR]

        def column(j):
            bias = b_ref[2:3, cols]
            left, tot = state["left"], state["tot"]
            mid, right = rows_of(JU + 1 + j), rows_of(j + 1)
            for o in range(4):
                for p in PAIR:
                    m = mid[o][p] + bias
                    for bc, side in zip(PAIR, (left, right)):
                        ob = (side[o][p] + m).astype(BF)
                        u_ref[p, 4 * q + o, 2 * j + bc, :, cols] = ob
                        v = ob.astype(F32).reshape(2, 8, LANES)
                        tot[p][0] += jnp.sum(v, axis=0)
                        tot[p][1] += jnp.sum(v * v, axis=0)
            state["left"] = right

        def finish():
            for p in PAIR:
                for z in PAIR:
                    st_ref[p, z, :, cols] += state["tot"][p][z]

        return [start] + [functools.partial(column, j) for j in range(JU)] + [finish]

    def body(accE, accF):
        combine = sum([combine_items(q, half) for q in PAIR for half in PAIR], [])

        @pl.when(t == 0)
        def _():
            weights.start()
            for q in PAIR:
                for a in accE[0][q] + accE[1][q] + accF[q]:
                    pltpu.matmul_pop(a)
            for f in PAIR:
                for r in list(range(PADR)) + list(range(PADR + HU, HPU)):
                    xs[f * HPU + r] = jnp.zeros((JU + 2, S, C), BF)
            fill(1, xb_ref)
            if from_halo:
                @pl.when(first_ref[0] == 1)
                def _():
                    fill(0, xb_ref)

                @pl.when(first_ref[0] == 0)
                def _():
                    fill(0, xa_ref)
            else:
                fill(0, xa_ref)
            weights.wait()

        @pl.when(t == 2)
        def _():
            st_ref[...] = jnp.zeros_like(st_ref)

        @pl.when(t < last)
        def _():
            spread(mxu_items(accE, accF), combine, 12)

        @pl.when(t == last)
        def _():
            for g in combine:
                g()

    refs = lambda tiles: [[pltpu.ACC(q)((tiles * S, C), F32) for _ in range(4)] for q in PAIR]
    pl.run_scoped(body, [refs(JU + 1), refs(JU + 1)], refs(JU))


def up_conv(a, c, w27, b, first, from_halo):
    (xa, ka), (xb, kb) = a, c
    frame = (1, HU, JU, S, C)
    return pl.pallas_call(
        functools.partial(up_body, from_halo),
        grid=(HU // 4 + 2,),
        in_specs=[SMEM, whole(5, C), whole(*frame, lead=ka), whole(*frame, lead=kb), ANY],
        out_specs=[pl.BlockSpec((2, 8, 2 * JU, S, C), lambda t: (0, jnp.clip(t - 2, 0, HU // 4 - 1), 0, 0, 0)), whole(2, 2, 8, C)],
        out_shape=[sds(2, 2 * HU, 2 * JU, S, C), sds(2, 2, 8, C, dtype=F32)],
        scratch_shapes=[pltpu.VMEM((2 * HPU, JU + 2, S, C), BF), pltpu.VMEM((NS, 2, 3, 2, 2, 2 * JU + 1, S, C), F32)] + WEIGHTS,
        compiler_params=params(46),
        cost_estimate=cost(4 * HU * JU * S * C * TAPS * C, 10 * HU * JU * S * C),
    )(first, b, xa, xb, w27)


def prep_body(z_ref, z0_ref, z1_ref, st_ref, tmp):
    @pl.when(pl.program_id(0) == 0)
    def _():
        st_ref[...] = jnp.zeros_like(st_ref)

    for f in PAIR:
        for r in range(z_ref.shape[1]):
            v = z_ref[f, r].astype(F32)
            add_sums(st_ref, f, v)
            for half, cols in zip(PAIR, BOTH):
                tmp[f, r, half] = v[:, cols]
        for r in range(z_ref.shape[1]):
            for j in range(JU):
                for half, cols in zip(PAIR, BOTH):
                    (z0_ref, z1_ref)[f][0, r, j, :, cols] = tmp[f, r, half, pl.ds(j, S, stride=JU), :].astype(BF)


def prep(z):
    rows, width = 8, JU * S
    return pl.pallas_call(
        prep_body,
        grid=(HU // rows,),
        in_specs=[pl.BlockSpec((2, rows, width, C), lambda t: (0, t, 0, 0))],
        out_specs=[pl.BlockSpec((1, rows, JU, S, C), lambda t: (0, t, 0, 0, 0))] * 2 + [whole(2, 2, 8, C)],
        out_shape=[sds(1, HU, JU, S, C)] * 2 + [sds(2, 2, 8, C, dtype=F32)],
        scratch_shapes=[pltpu.VMEM((2, rows, 2, width, LANES), F32)],
        compiler_params=params(46),
        cost_estimate=cost(8 * z.size, 4 * z.size),
        name="prep",
    )(z)


def stats_body(n, gi, cnt, drop, *refs):
    sts, (gamma_ref, beta_ref, gn_ref, mine, chip, recv, send_sem, recv_sem) = refs[:n], refs[n:]
    me = lax.axis_index("t")
    mate = me + 1 - 2 * lax.rem(me, 2)
    barrier = pltpu.get_barrier_semaphore()
    for d in range(1, 4):
        pl.semaphore_signal(barrier, inc=1, device_id={"t": lax.rem(me + d, 4)}, device_id_type=MESH)
    keep = jnp.where(me == 0, 0.0, 1.0) if drop else 1.0
    for z in PAIR:
        tot = None
        for st in sts:
            for f in range(st.shape[0]):
                v = st[f, z]
                if drop and st is sts[0] and f == 0:
                    v = v * keep
                tot = v if tot is None else tot + v
        mine[z] = tot
    pl.semaphore_wait(barrier, 3)

    def copy(src, slot, dev, sem):
        return pltpu.make_async_remote_copy(
            src_ref=src, dst_ref=recv.at[slot], send_sem=send_sem.at[sem], recv_sem=recv_sem.at[slot],
            device_id={"t": dev}, device_id_type=MESH)

    swap = copy(mine, 0, mate, 0)
    swap.start()
    swap.wait()
    chip[...] = mine[...] + recv[0]

    @pl.when(me == 0)
    def _():
        out = [copy(chip, 1, 2, 1), copy(chip, 1, 3, 2)]
        for c in out:
            c.start()
        for c in out:
            c.wait_send()

    @pl.when(me >= 2)
    def _():
        c = copy(chip, 1, me - 2, 1)
        c.start()
        c.wait_send()

    copy(chip, 1, mate, 1).wait_recv()
    both = jnp.sum(chip[...] + recv[1], axis=1)
    s = jnp.concatenate([both, jnp.zeros((6, C), F32)], axis=0)
    lane = lax.broadcasted_iota(jnp.int32, s.shape, 1)
    for d in (1, 2, 4):
        s = s + jnp.where((lane & d) == 0, pltpu.roll(s, C - d, 1), pltpu.roll(s, d, 1))
    mean = s[0:1] / cnt
    inv = lax.rsqrt(s[1:2] / cnt - mean * mean + EPS)
    gn_ref[...] = jnp.zeros_like(gn_ref)
    gn_ref[0:1, :] = mean
    gn_ref[1:2, :] = inv * gamma_ref[gi:gi + 1, :]
    gn_ref[2:3, :] = beta_ref[gi:gi + 1, :]


def stats(sts, gamma, beta, gi, cnt, drop=False):
    part = pltpu.VMEM((2, 8, C), F32)
    return pl.pallas_call(
        functools.partial(stats_body, len(sts), gi, float(cnt), drop),
        in_specs=[VMEM] * (len(sts) + 2),
        out_specs=VMEM,
        out_shape=sds(8, C, dtype=F32),
        scratch_shapes=[part, part, pltpu.VMEM((2, 2, 8, C), F32), pltpu.SemaphoreType.DMA((3,)), pltpu.SemaphoreType.DMA((2,))],
        compiler_params=pltpu.CompilerParams(collective_id=gi, has_side_effects=True, vmem_limit_bytes=46 * 2**20),
    )(*sts, gamma, beta)


def solution(mesh):
    nt = mesh.shape['t']

    hbm = lambda x: pltpu.with_memory_space_constraint(x, pltpu.HBM)

    def send(x):
        return lax.ppermute(x, 't', [(i, i + 1) for i in range(nt - 1)])

    def local(z, w, b, gamma, beta):
        first = (lax.axis_index('t') == 0).astype(jnp.int32).reshape(1)
        w27 = w.reshape(-1, TAPS, C, C)
        cnt1 = nt * z.size // GROUPS
        cnt2 = (2 * 2 * nt - 1) * 4 * z.size // (2 * GROUPS)
        run = lambda frames, gn, wi, **kw: conv(frames, w27, b, gn, first, wi, **kw)
        z0, z1, st = prep(hbm(z))
        zb = send(z1)
        za = send(z0)
        gn = stats([st], gamma, beta, 0, cnt1)
        h1, st1 = run([(zb, 0), (z0, 0), (z1, 0)], gn, 0, nsub=1)
        hb = send(h1)
        h0, st0 = run([(za, 0), (zb, 0), (z0, 0)], gn, 0, nsub=2)
        ha = send(h0)
        gn = stats([st0, st1], gamma, beta, 1, cnt1)
        x1, _ = run([(hb, 0), (h0, 0), (h1, 0)], gn, 1, nsub=1, res=[(z1, 0)])
        xh = send(x1)
        x0, _ = run([(ha, 0), (hb, 0), (h0, 0)], gn, 1, nsub=2, res=[(z0, 0)])
        u23, st23 = up_conv((x0, 0), (x1, 0), w27, b, first, False)
        uh = send(u23)
        u01, st01 = up_conv((xh, 0), (x0, 0), w27, b, first, True)
        gn = stats([st01, st23], gamma, beta, 2, cnt2, drop=True)
        pair = lambda lo, hi: [(lo, 0), (lo, 1), (hi, 0), (hi, 1)]
        h23, st23 = run(pair(u01, u23), gn, 3)
        hh = send(h23)
        h01, st01 = run(pair(uh, u01), gn, 3, nsub=2)
        gn = stats([st01, st23], gamma, beta, 3, cnt2, drop=True)
        y = run(pair(h01, h23), gn, 4, res=[(u23, 0), (u23, 1)], natural=True)
        return run(pair(hh, h01), gn, 4, nsub=2, res=[(u01, 0), (u01, 1)], natural=True, ybuf=y)

    spec = P(('batch', 't'))

    return jax.shard_map(local, mesh=mesh, in_specs=(spec, P(), P(), P(), P()), out_specs=spec, check_vma=False)
```
